32 devices in a mesh: dp: 4 (over y, z), ep: 8 (over x, core).
Axes of the slice: x: 4, y: 2, z: 2, core: 2. Of those that a mesh axis runs over, the one named last changes fastest.
The devices are a block of a 4x4x8 slice.
Arguments:
- tokens: bfloat16 [32768, 2048], P(('dp', 'ep')), parts along dimension 0
- w_router: bfloat16 [2048, 64], replicated
- expert_ids: int32 [32768, 6], P(('dp', 'ep')), parts along dimension 0
- w_gate: bfloat16 [64, 2048, 1408], P('ep')
- w_up: bfloat16 [64, 2048, 1408], P('ep')
- w_down: bfloat16 [64, 1408, 2048], P('ep')
- shared_gate: bfloat16 [2048, 2816], replicated
- shared_up: bfloat16 [2048, 2816], replicated
- shared_down: bfloat16 [2816, 2048], replicated
Outputs:
- output: bfloat16 [32768, 2048], P(('dp', 'ep')), parts along dimension 0
There are 4 independent parts. The reference program is written for one: setup_inputs(seed, part) draws one part's arguments, and reference() takes and returns one part's arrays. A program takes and returns all parts, laid end to end along the dimension named above; an argument that names none is the same for every part.
All inputs are finite; a program needn't handle non-finite values.
Results may differ from the reference program's by a relative error of at most 0.00812481.
Values are sent between devices in bfloat16 or wider.
A program may use at most 768 MiB of HBM per device.

```python
import jax
import jax.numpy as jnp
from jax import lax

MODEL_DIM = 2048
EXPERT_FF = 1408
SHARED_FF = 2816
NUM_EXPERTS = 64
TOP_K = 6
TOKENS_DEV = 1024
GROUP_SIZE = 8

NUM_TOKENS = GROUP_SIZE * TOKENS_DEV
NUM_PAIRS = NUM_TOKENS * TOP_K
BASE_LOAD = TOKENS_DEV * TOP_K // NUM_EXPERTS
CAPACITY = BASE_LOAD + BASE_LOAD // 2 + min(TOKENS_DEV * TOP_K % NUM_EXPERTS, 1)
EXPERT_ROWS = GROUP_SIZE * CAPACITY


def draw_routing(rng_key):
    perm_key, delta_key, tok_key, rot_key = jax.random.split(rng_key, 4)
    spread = BASE_LOAD // 2
    expert_range = jnp.arange(NUM_EXPERTS, dtype=jnp.int32)
    deltas = jax.random.randint(delta_key, (GROUP_SIZE, NUM_EXPERTS // 2), 0, spread + 1, dtype=jnp.int32)
    deltas = deltas.at[:, 0].set(spread)
    signed_delta = jnp.stack([deltas, -deltas], axis=-1).reshape(GROUP_SIZE, NUM_EXPERTS)
    extra_one = (expert_range < TOKENS_DEV * TOP_K % NUM_EXPERTS).astype(jnp.int32)
    dev_counts = BASE_LOAD + extra_one[None, :] + signed_delta
    labels = jax.random.permutation(perm_key, NUM_EXPERTS).astype(jnp.int32)
    pair_range = jnp.arange(TOKENS_DEV * TOP_K, dtype=jnp.int32)

    def one_device(counts, perm_seed, rot_seed):
        run_ends = jnp.cumsum(counts)
        sequence = jnp.searchsorted(run_ends, pair_range, side='right').astype(jnp.int32)
        slot_table = sequence.reshape(TOP_K, TOKENS_DEV).T
        slot_table = slot_table[jax.random.permutation(perm_seed, TOKENS_DEV)]
        rot_shift = jax.random.randint(rot_seed, (TOKENS_DEV, 1), 0, TOP_K, dtype=jnp.int32)
        col_order = (jnp.arange(TOP_K, dtype=jnp.int32)[None, :] + rot_shift) % TOP_K
        slot_table = jnp.take_along_axis(slot_table, col_order, axis=1)
        return labels[slot_table]

    routed_ids = jax.vmap(one_device)(dev_counts, jax.random.split(tok_key, GROUP_SIZE), jax.random.split(rot_key, GROUP_SIZE))
    return routed_ids.reshape(NUM_TOKENS, TOP_K)


def normal_weight(rng_key, shape, scale):
    return (jax.random.normal(rng_key, shape, jnp.float32) * scale).astype(jnp.bfloat16)


def setup_inputs(seed: int = 0, part: int = 0) -> dict:
    base_key = jax.random.key(seed)
    part_key = jax.random.fold_in(base_key, part)
    weight_keys = jax.random.split(base_key, 7)
    part_keys = jax.random.split(part_key, 2)
    in_scale = MODEL_DIM ** -0.5
    tokens = jax.random.normal(part_keys[0], (NUM_TOKENS, MODEL_DIM), jnp.float32).astype(jnp.bfloat16)
    return {
        'tokens': tokens,
        'w_router': normal_weight(weight_keys[0], (MODEL_DIM, NUM_EXPERTS), 2.0 * in_scale),
        'expert_ids': draw_routing(part_keys[1]),
        'w_gate': normal_weight(weight_keys[1], (NUM_EXPERTS, MODEL_DIM, EXPERT_FF), in_scale),
        'w_up': normal_weight(weight_keys[2], (NUM_EXPERTS, MODEL_DIM, EXPERT_FF), in_scale),
        'w_down': normal_weight(weight_keys[3], (NUM_EXPERTS, EXPERT_FF, MODEL_DIM), EXPERT_FF ** -0.5),
        'shared_gate': normal_weight(weight_keys[4], (MODEL_DIM, SHARED_FF), in_scale),
        'shared_up': normal_weight(weight_keys[5], (MODEL_DIM, SHARED_FF), in_scale),
        'shared_down': normal_weight(weight_keys[6], (SHARED_FF, MODEL_DIM), SHARED_FF ** -0.5),
    }


def swiglu(rows_in, w_one, w_three, w_two):
    gate_act = jnp.dot(rows_in, w_one, preferred_element_type=jnp.float32)
    up_act = jnp.dot(rows_in, w_three, preferred_element_type=jnp.float32)
    hidden = (jax.nn.silu(gate_act) * up_act).astype(jnp.bfloat16)
    return jnp.dot(hidden, w_two, preferred_element_type=jnp.float32).astype(jnp.bfloat16)


def reference(tokens, w_router, expert_ids, w_gate, w_up, w_down, shared_gate, shared_up, shared_down):
    logits = jnp.dot(tokens, w_router, preferred_element_type=jnp.float32)
    picked = jnp.take_along_axis(logits, expert_ids, axis=1)
    gate_vals = jax.nn.softmax(picked, axis=-1)
    flat_ids = expert_ids.reshape(-1)
    sort_order = jnp.argsort(flat_ids, stable=True)
    counts = jnp.bincount(flat_ids, length=NUM_EXPERTS)
    starts = jnp.cumsum(counts) - counts
    row_range = jnp.arange(EXPERT_ROWS)
    src_pos = jnp.minimum(starts[:, None] + row_range[None, :], NUM_PAIRS - 1)
    is_valid = row_range[None, :] < counts[:, None]
    pair_id = sort_order[src_pos]
    tok_table = jnp.where(is_valid, pair_id // TOP_K, NUM_TOKENS)
    gate_table = jnp.where(is_valid, gate_vals.reshape(-1)[pair_id], 0.0)
    shared_out = swiglu(tokens, shared_gate, shared_up, shared_down)

    def expert_step(running, step_in):
        rows_tok, rows_gate, w_one, w_three, w_two = step_in
        rows_in = jnp.take(tokens, rows_tok, axis=0, mode='fill', fill_value=0)
        out_rows = swiglu(rows_in, w_one, w_three, w_two)
        running = running.at[rows_tok].add(rows_gate[:, None] * out_rows.astype(jnp.float32), mode='drop')
        return running, None

    summed, unused_tail = lax.scan(expert_step, shared_out.astype(jnp.float32), (tok_table, gate_table, w_gate, w_up, w_down))
    return summed.astype(jnp.bfloat16)
```

```python
import functools

import jax
import jax.numpy as jnp
from jax import lax
from jax.experimental import pallas as pl
from jax.experimental.pallas import tpu as pltpu
from jax.sharding import PartitionSpec as P


LANES = 128
BLOCK_ROWS = 256
SLAB = 24
CHUNK = 256


def capacity_of(tok_dev, top_k, num_exp):
    base_load = tok_dev * top_k // num_exp
    return base_load + base_load // 2 + min(tok_dev * top_k % num_exp, 1)


def experts_kernel(table_cap, num_after, count_s, tok_s, gate_s, seg_a, seg_b, seg_c, seg_d, w_gate, w_up, w_down, *refs):
    (out_mine, out_other, tok_v, acc, buf_g, buf_u, buf_d, slab_v, rows_v, hid_v,
     sem_tok, sem_g, sem_u, sem_d, sem_out) = refs[num_after:]
    num_loc, model_dim, ff_dim = w_gate.shape
    half = seg_a.shape[0]
    pieces = seg_a.shape[1]
    num_rows = 4 * half

    def load_gu(exp):
        slot = lax.rem(exp, 2)
        return (pltpu.make_async_copy(w_gate.at[exp], buf_g.at[slot], sem_g.at[slot]),
                pltpu.make_async_copy(w_up.at[exp], buf_u.at[slot], sem_u.at[slot]))

    def load_d(exp):
        return pltpu.make_async_copy(w_down.at[exp], buf_d, sem_d)

    seg_copies = [pltpu.make_async_copy(seg, tok_v.at[pl.ds(half * idx, half)], sem_tok.at[idx])
                  for idx, seg in enumerate((seg_a, seg_b, seg_c, seg_d))]
    for copy in seg_copies:
        copy.start()
    for copy in load_gu(0):
        copy.start()
    load_d(0).start()

    def clear(idx, carry):
        acc[pl.ds(idx * 8, 8)] = jnp.zeros((8, pieces, LANES), jnp.float32)
        return carry

    lax.fori_loop(0, num_rows // 8, clear, 0)
    tok_v[num_rows] = jnp.zeros((pieces, LANES), jnp.bfloat16)
    acc[num_rows] = jnp.zeros((pieces, LANES), jnp.float32)
    for copy in seg_copies:
        copy.wait()

    def expert(exp, carry):
        slot = lax.rem(exp, 2)

        @pl.when(exp + 1 < num_loc)
        def _():
            for copy in load_gu(exp + 1):
                copy.start()

        count = count_s[exp]
        num_blocks = jnp.maximum((count + BLOCK_ROWS - 1) // BLOCK_ROWS, 1)

        def block(blk, carry):
            base = exp * table_cap + blk * BLOCK_ROWS
            groups = (jnp.minimum(count - blk * BLOCK_ROWS, BLOCK_ROWS) + 7) // 8

            def fetch(grp, carry):
                for lane in range(8):
                    row = grp * 8 + lane
                    slab_v[pl.ds(pl.multiple_of(row * SLAB, 8), pieces), :] = tok_v[tok_s[base + row]].astype(jnp.float32)
                return carry

            lax.fori_loop(0, groups, fetch, 0)
            for col in range(pieces):
                rows_v[:, col * LANES:(col + 1) * LANES] = slab_v[pl.ds(col, BLOCK_ROWS, stride=SLAB), :].astype(jnp.bfloat16)

            @pl.when(blk == 0)
            def _():
                for copy in load_gu(exp):
                    copy.wait()

            for start in range(0, ff_dim, CHUNK):
                width = min(CHUNK, ff_dim - start)
                cols = slice(start, start + width)
                gate_act = jnp.dot(rows_v[...], buf_g[slot, :, cols], preferred_element_type=jnp.float32)
                up_act = jnp.dot(rows_v[...], buf_u[slot, :, cols], preferred_element_type=jnp.float32)
                hid_v[:, cols] = (jax.nn.silu(gate_act) * up_act).astype(jnp.bfloat16)

            @pl.when(blk == 0)
            def _():
                load_d(exp).wait()

            for start in range(0, model_dim, CHUNK):
                out_rows = jnp.dot(hid_v[...], buf_d[:, start:start + CHUNK], preferred_element_type=jnp.float32)
                out_rows = out_rows.astype(jnp.bfloat16).astype(jnp.float32)
                for off in range(0, CHUNK, LANES):
                    slab_v[pl.ds((start + off) // LANES, BLOCK_ROWS, stride=SLAB), :] = out_rows[:, off:off + LANES]

            @pl.when((blk == num_blocks - 1) & (exp + 1 < num_loc))
            def _():
                load_d(exp + 1).start()

            def combine(grp, carry):
                toks, sums = [], []
                for lane in range(8):
                    row = grp * 8 + lane
                    tok = tok_s[base + row]
                    piece = slab_v[pl.ds(pl.multiple_of(row * SLAB, 8), pieces), :]
                    toks.append(tok)
                    sums.append(acc[tok] + gate_s[base + row] * piece)
                for tok, val in zip(toks, sums):
                    acc[tok] = val
                return carry

            lax.fori_loop(0, groups, combine, 0)
            return carry

        lax.fori_loop(0, num_blocks, block, 0)
        return carry

    lax.fori_loop(0, num_loc, expert, 0)
    outs = [pltpu.make_async_copy(acc.at[pl.ds(2 * half * idx, 2 * half)], out, sem_out.at[idx])
            for idx, out in enumerate((out_mine, out_other))]
    for copy in outs:
        copy.start()
    for copy in outs:
        copy.wait()


def expert_pass(counts, toks, gates, segs, w_gate, w_up, w_down, table_cap, after):
    num_loc, model_dim, ff_dim = w_gate.shape
    half, pieces, _ = segs[0].shape
    num_rows = 4 * half
    out_type = jax.ShapeDtypeStruct((2 * half, pieces, LANES), jnp.float32)
    any_spec = pl.BlockSpec(memory_space=pl.ANY)
    smem_spec = pl.BlockSpec(memory_space=pltpu.SMEM)
    avg_rows = num_rows * 6 // 8
    return pl.pallas_call(
        functools.partial(experts_kernel, table_cap, len(after)),
        out_shape=(out_type, out_type),
        in_specs=[smem_spec] * 3 + [any_spec] * (7 + len(after)),
        out_specs=(any_spec, any_spec),
        scratch_shapes=[
            pltpu.VMEM((num_rows + 8, pieces, LANES), jnp.bfloat16),
            pltpu.VMEM((num_rows + 8, pieces, LANES), jnp.float32),
            pltpu.VMEM((2, model_dim, ff_dim), jnp.bfloat16),
            pltpu.VMEM((2, model_dim, ff_dim), jnp.bfloat16),
            pltpu.VMEM((ff_dim, model_dim), jnp.bfloat16),
            pltpu.VMEM((BLOCK_ROWS * SLAB, LANES), jnp.float32),
            pltpu.VMEM((BLOCK_ROWS, model_dim), jnp.bfloat16),
            pltpu.VMEM((BLOCK_ROWS, ff_dim), jnp.bfloat16),
            pltpu.SemaphoreType.DMA((4,)),
            pltpu.SemaphoreType.DMA((2,)),
            pltpu.SemaphoreType.DMA((2,)),
            pltpu.SemaphoreType.DMA,
            pltpu.SemaphoreType.DMA((2,)),
        ],
        compiler_params=pltpu.CompilerParams(vmem_limit_bytes=63 * 1024 * 1024),
        cost_estimate=pl.CostEstimate(flops=6 * avg_rows * model_dim * ff_dim * 3 // 2, transcendentals=0,
                                      bytes_accessed=3 * num_loc * model_dim * ff_dim * 2),
        name='experts',
    )(counts, toks, gates, *segs, w_gate, w_up, w_down, *after)


def finish_kernel(blocks_half, shared_ref, mine_ref, other_ref, near_a, near_b, far_a, far_b, out_ref, sum_v):
    rows = shared_ref.shape[0]
    pieces = mine_ref.shape[1]
    idx = pl.program_id(0)
    flat = (rows * pieces, LANES)

    def gather_sum(near, far):
        total = (mine_ref[...] + other_ref[...]) + (near[...] + far[...])
        sum_v[...] = total.reshape(flat)

    pl.when(idx < blocks_half)(lambda: gather_sum(near_a, far_a))
    pl.when(idx >= blocks_half)(lambda: gather_sum(near_b, far_b))
    for col in range(pieces):
        cols = slice(col * LANES, (col + 1) * LANES)
        out_ref[:, cols] = (shared_ref[:, cols].astype(jnp.float32) + sum_v[pl.ds(col, rows, stride=pieces), :]).astype(jnp.bfloat16)


def finish(shared_out, mine, other, near_a, near_b, far_a, far_b):
    tok_dev, model_dim = shared_out.shape
    pieces = mine.shape[1]
    rows = 128
    blocks_half = tok_dev // rows // 2
    full = lambda idx: (idx, 0, 0)
    first = lambda idx: (jnp.minimum(idx, blocks_half - 1), 0, 0)
    second = lambda idx: (jnp.maximum(idx - blocks_half, 0), 0, 0)
    slab = (rows, pieces, LANES)
    return pl.pallas_call(
        functools.partial(finish_kernel, blocks_half),
        out_shape=jax.ShapeDtypeStruct((tok_dev, model_dim), jnp.bfloat16),
        grid=(tok_dev // rows,),
        in_specs=[pl.BlockSpec((rows, model_dim), lambda idx: (idx, 0)), pl.BlockSpec(slab, full), pl.BlockSpec(slab, full),
                  pl.BlockSpec(slab, first), pl.BlockSpec(slab, second), pl.BlockSpec(slab, first), pl.BlockSpec(slab, second)],
        out_specs=pl.BlockSpec((rows, model_dim), lambda idx: (idx, 0)),
        scratch_shapes=[pltpu.VMEM((rows * pieces, LANES), jnp.float32)],
        compiler_params=pltpu.CompilerParams(vmem_limit_bytes=48 * 1024 * 1024),
        cost_estimate=pl.CostEstimate(flops=tok_dev * model_dim * 8, transcendentals=0, bytes_accessed=tok_dev * model_dim * 20),
        name='finish',
    )(shared_out, mine, other, near_a, near_b, far_a, far_b)


def shared_hidden(tok_rows, shared_gate, shared_up):
    gate_act = jnp.dot(tok_rows, shared_gate, preferred_element_type=jnp.float32)
    up_act = jnp.dot(tok_rows, shared_up, preferred_element_type=jnp.float32)
    return (jax.nn.silu(gate_act) * up_act).astype(jnp.bfloat16)


def routing_exchange(tok_rows, w_router, ids_loc):
    top_k = ids_loc.shape[1]
    num_exp = w_router.shape[1]
    logits = lax.dot_general(w_router, tok_rows, (((0,), (1,)), ((), ())), preferred_element_type=jnp.float32)
    ids = ids_loc.T
    exp_range = jnp.arange(num_exp, dtype=jnp.int32)[:, None]
    picked = jnp.stack([jnp.sum(jnp.where(ids[k][None, :] == exp_range, logits, 0.0), axis=0) for k in range(top_k)])
    gates = jax.nn.softmax(picked, axis=0)
    packed = jnp.concatenate([ids.astype(jnp.float32), gates], axis=0)
    return lax.all_gather(packed, 'ep')


def routing_tables(everyone, num_exp, group, table_cap):
    top_k, tok_dev = everyone.shape[1] // 2, everyone.shape[2]
    num_loc = num_exp // group
    half = tok_dev // 2
    me = lax.axis_index('ep')
    chip, core = me // 2, me % 2
    chips = group // 2
    order = [((chip + off) % chips) * 2 + side for off in range(chips) for side in (core, 1 - core)]
    rolled = jnp.stack([lax.dynamic_index_in_dim(everyone, src, 0, keepdims=False) for src in order])
    mine = (me * num_loc + jnp.arange(num_loc, dtype=jnp.int32)).astype(jnp.float32)[None, :, None]
    named = jnp.zeros((group, num_loc, tok_dev), jnp.bool_)
    gate = jnp.zeros((group, num_loc, tok_dev), jnp.float32)
    for k in range(top_k):
        hit = rolled[:, k][:, None, :] == mine
        named = named | hit
        gate = gate + jnp.where(hit, rolled[:, top_k + k][:, None, :], 0.0)
    segs = [[(6, 0), (2, 1), (7, 0), (3, 1)],
            [(4, 0), (4, 1), (5, 0), (5, 1)],
            [(6, 1), (2, 0), (7, 1), (3, 0)],
            [(0, 0), (0, 1), (1, 0), (1, 1)]]

    def arrange(table):
        return jnp.stack([jnp.concatenate([table[src, :, side * half:(side + 1) * half] for src, side in seg], axis=1) for seg in segs])

    named, gate = arrange(named), arrange(gate)
    num_rows = 2 * tok_dev
    key = jnp.where(named, jnp.arange(num_rows, dtype=jnp.int32), num_rows)
    counts = jnp.sum(named.astype(jnp.int32), axis=2)
    key, gate = lax.sort((key, gate), dimension=2, num_keys=1, is_stable=False)
    flat = (len(segs), num_loc * table_cap)
    return counts, key[:, :, :table_cap].reshape(flat), gate[:, :, :table_cap].reshape(flat)


def solution(mesh):
    group = mesh.shape['ep']
    row_spec = P(('dp', 'ep'), None)
    full_spec = P(None, None)
    expert_spec = P('ep', None, None)
    forward = [(dev, (dev + 2) % group) for dev in range(group)]
    backward = [(dev, (dev - 2) % group) for dev in range(group)]
    across = [(dev, dev ^ 1) for dev in range(group)]

    def send(array, route):
        return lax.ppermute(array, 'ep', route)

    def device_step(tok_rows, w_router, ids_loc, w_gate, w_up, w_down, shared_gate, shared_up, shared_down):
        tok_dev, model_dim = tok_rows.shape
        top_k = ids_loc.shape[1]
        num_exp = w_router.shape[1]
        half = tok_dev // 2
        pieces = model_dim // LANES
        worst = 4 * capacity_of(tok_dev, top_k, num_exp)
        table_cap = -(-worst // BLOCK_ROWS) * BLOCK_ROWS

        slabs = tok_rows.reshape(tok_dev, pieces, LANES)
        own_a, own_b = slabs[:half], slabs[half:]
        everyone = routing_exchange(tok_rows, w_router, ids_loc)
        own_a, own_b, everyone = lax.optimization_barrier((own_a, own_b, everyone))
        left_a = send(own_a, forward)
        right_b = send(own_b, backward)
        pair_a, pair_b = send(own_a, across), send(own_b, across)

        counts, toks, gates = routing_tables(everyone, num_exp, group, table_cap)

        def run(idx, segs, after):
            mine, other = expert_pass(counts[idx], toks[idx], gates[idx], segs, w_gate, w_up, w_down, table_cap, after)
            return mine, send(other, across)

        hidden = shared_hidden(tok_rows, shared_gate, shared_up)
        far_a, far_b = send(left_a, forward), send(right_b, backward)
        left_b, right_a = send(own_b, forward), send(own_a, backward)

        segs = [left_a, right_b, send(left_a, across), send(right_b, across)]
        mine, other = run(0, segs, [hidden])
        shared_out = jnp.dot(hidden, shared_down, preferred_element_type=jnp.float32).astype(jnp.bfloat16)
        to_left, to_right = mine[:half] + other[:half], mine[half:] + other[half:]
        near_a, near_b = send(to_left, backward), send(to_right, forward)

        segs = [far_a, far_b, send(far_a, across), send(far_b, across)]
        mine, other = run(1, segs, [to_left, to_right, shared_out])
        to_right, to_left = mine[:half] + other[:half], mine[half:] + other[half:]
        via_a, via_b = send(to_right, forward), send(to_left, backward)

        segs = [left_b, right_a, send(left_b, across), send(right_a, across)]
        mine, other = run(2, segs, [to_left, to_right])
        to_left, to_right = mine[:half] + other[:half] + via_b, mine[half:] + other[half:] + via_a
        last_b, last_a = send(to_left, backward), send(to_right, forward)

        mine, other = run(3, [own_a, own_b, pair_a, pair_b], [to_left, to_right])
        return finish(shared_out, mine, other, near_a, near_b, last_a, last_b)

    return jax.shard_map(device_step, mesh=mesh, in_specs=(row_spec, full_spec, row_spec, expert_spec, expert_spec, expert_spec, full_spec, full_spec, full_spec), out_specs=row_spec, check_vma=False)
```

```python
import functools

import jax
import jax.numpy as jnp
from jax import lax
from jax.experimental import pallas as pl
from jax.experimental.pallas import tpu as pltpu
from jax.sharding import PartitionSpec as P


LANES = 128
ROW_SIZES = (160, 208, 256, 320)
MANY_ROWS = ROW_SIZES[-1]
PITCH = MANY_ROWS + 12
SLAB = 24
CHUNK = 256
SLOTS = 3


def capacity_of(tok_dev, top_k, num_exp):
    base_load = tok_dev * top_k // num_exp
    return base_load + base_load // 2 + min(tok_dev * top_k % num_exp, 1)


def experts_kernel(list_cap, num_after, count_s, tok_s, gate_s, seg_a, seg_b, seg_c, seg_d, w_gate, w_up, w_down, *refs):
    (*outs, tok_v, acc, buf_g, buf_u, buf_d, slab_v, rows_v, hid_v,
     sem_tok, sem_g, sem_u, sem_d, sem_out) = refs[num_after:]
    slots, width = buf_d.shape[:2]
    num_loc, model_dim, ff_dim = w_gate.shape
    half = seg_a.shape[0]
    pieces = seg_a.shape[1]
    segs = (seg_a, seg_b, seg_c, seg_d)
    num_segs = len(segs)
    num_rows = num_segs * half

    parts = [(start, min(width, ff_dim - start)) for start in range(0, ff_dim, width)]

    def load(stage, part):
        exp, slot = stage // len(parts), lax.rem(stage, slots)
        start, cols = parts[part]
        return (pltpu.make_async_copy(w_gate.at[exp, :, pl.ds(start, cols)], buf_g.at[slot, :, pl.ds(0, cols)], sem_g.at[slot]),
                pltpu.make_async_copy(w_up.at[exp, :, pl.ds(start, cols)], buf_u.at[slot, :, pl.ds(0, cols)], sem_u.at[slot]),
                pltpu.make_async_copy(w_down.at[exp, pl.ds(start, cols)], buf_d.at[slot, pl.ds(0, cols)], sem_d.at[slot]))

    seg_copies = [pltpu.make_async_copy(seg, tok_v.at[pl.ds(half * idx, half)], sem_tok.at[idx]) for idx, seg in enumerate(segs)]
    for copy in seg_copies:
        copy.start()
    for copy in load(0, 0):
        copy.start()

    def clear(idx, carry):
        acc[pl.ds(idx * 8, 8)] = jnp.zeros((8, pieces, LANES), jnp.float32)
        return carry

    lax.fori_loop(0, num_rows // 8, clear, 0)
    tok_v[num_rows] = jnp.zeros((pieces, LANES), jnp.bfloat16)
    acc[num_rows] = jnp.zeros((pieces, LANES), jnp.float32)
    for copy in seg_copies:
        copy.wait()
    for stage in range(1, slots):
        for copy in load(stage, stage % len(parts)):
            copy.start()

    def unpack(rows):
        for col in range(pieces):
            rows_v[:rows, col * LANES:(col + 1) * LANES] = slab_v[col * PITCH:col * PITCH + rows, :].astype(jnp.bfloat16)

    def multiply(slot, part, rows):
        cols = parts[part][1]
        if part == 0:
            unpack(rows)
        for start in range(0, cols, CHUNK):
            span = slice(start, min(start + CHUNK, cols))
            gate_act = jnp.dot(rows_v[:rows], buf_g[slot, :, span], preferred_element_type=jnp.float32)
            up_act = jnp.dot(rows_v[:rows], buf_u[slot, :, span], preferred_element_type=jnp.float32)
            hid_v[:rows, span] = (jax.nn.silu(gate_act) * up_act).astype(jnp.bfloat16)
        for start in range(0, model_dim, CHUNK):
            out_rows = jnp.dot(hid_v[:rows, :cols], buf_d[slot, :cols, start:start + CHUNK], preferred_element_type=jnp.float32)
            for off in range(0, CHUNK, LANES):
                place = pl.ds((start + off) // LANES * PITCH, rows)
                piece = out_rows[:, off:off + LANES]
                if part > 0:
                    piece = slab_v[place, :] + piece
                if part == len(parts) - 1:
                    piece = piece.astype(jnp.bfloat16).astype(jnp.float32)
                slab_v[place, :] = piece

    def expert(exp, carry):
        counts = [count_s[exp * num_segs + seg] for seg in range(num_segs)]
        total = functools.reduce(lambda left, right: left + right, counts)
        whole = total <= MANY_ROWS
        num_blocks = jnp.where(whole, 1, 2)

        def block(blk, carry):
            pair = num_segs // 2
            first = jnp.where(whole, 0, pair * blk)
            last = jnp.where(whole, num_segs, pair * blk + pair)
            rows = jnp.where(whole, total, jnp.where(blk == 0, counts[0] + counts[1], counts[2] + counts[3]))

            def lists(body):
                def one(seg, offset):
                    index = exp * num_segs + seg
                    base = index * list_cap
                    count = count_s[index]

                    def step(grp, carry):
                        body(base + grp * 8, offset + grp * 8)
                        return carry

                    lax.fori_loop(0, (count + 7) // 8, step, 0)
                    return offset + count

                lax.fori_loop(first, last, one, 0)

            def fetch(base, row):
                for lane in range(8):
                    slab_v[pl.ds(row + lane, pieces, stride=PITCH), :] = tok_v[tok_s[base + lane]].astype(jnp.float32)

            lists(fetch)

            for part in range(len(parts)):
                stage = exp * len(parts) + part
                slot = lax.rem(stage, slots)

                @pl.when(blk == 0)
                def _():
                    for copy in load(stage, part):
                        copy.wait()

                for low, size in zip((-1,) + ROW_SIZES[:-1], ROW_SIZES):
                    pl.when((rows > low) & (rows <= size))(functools.partial(multiply, slot, part, size))

                @pl.when((blk == num_blocks - 1) & (stage + slots < num_loc * len(parts)))
                def _():
                    for copy in load(stage + slots, (part + slots) % len(parts)):
                        copy.start()

            def combine(base, row):
                toks, sums = [], []
                for lane in range(8):
                    tok = tok_s[base + lane]
                    piece = slab_v[pl.ds(row + lane, pieces, stride=PITCH), :]
                    toks.append(tok)
                    sums.append(acc[tok] + gate_s[base + lane] * piece)
                for tok, val in zip(toks, sums):
                    acc[tok] = val

            lists(combine)
            return carry

        lax.fori_loop(0, num_blocks, block, 0)
        return carry

    lax.fori_loop(0, num_loc, expert, 0)
    out_copies = [pltpu.make_async_copy(acc.at[pl.ds(half * idx, half)], out, sem_out.at[idx]) for idx, out in enumerate(outs)]
    for copy in out_copies:
        copy.start()
    for copy in out_copies:
        copy.wait()


def expert_pass(counts, toks, gates, segs, w_gate, w_up, w_down, list_cap, after):
    num_loc, model_dim, ff_dim = w_gate.shape
    half, pieces, _ = segs[0].shape
    num_rows = 4 * half
    out_type = jax.ShapeDtypeStruct((half, pieces, LANES), jnp.float32)
    any_spec = pl.BlockSpec(memory_space=pl.ANY)
    smem_spec = pl.BlockSpec(memory_space=pltpu.SMEM)
    avg_rows = num_rows * 6 // 8
    part_dim = -(-ff_dim // (2 * CHUNK)) * CHUNK
    return pl.pallas_call(
        functools.partial(experts_kernel, list_cap, len(after)),
        out_shape=(out_type,) * len(segs),
        in_specs=[smem_spec] * 3 + [any_spec] * (7 + len(after)),
        out_specs=(any_spec,) * len(segs),
        scratch_shapes=[
            pltpu.VMEM((num_rows + 8, pieces, LANES), jnp.bfloat16),
            pltpu.VMEM((num_rows + 8, pieces, LANES), jnp.float32),
            pltpu.VMEM((SLOTS, model_dim, part_dim), jnp.bfloat16),
            pltpu.VMEM((SLOTS, model_dim, part_dim), jnp.bfloat16),
            pltpu.VMEM((SLOTS, part_dim, model_dim), jnp.bfloat16),
            pltpu.VMEM((pieces * PITCH, LANES), jnp.float32),
            pltpu.VMEM((MANY_ROWS, model_dim), jnp.bfloat16),
            pltpu.VMEM((MANY_ROWS, part_dim), jnp.bfloat16),
            pltpu.SemaphoreType.DMA((4,)),
            pltpu.SemaphoreType.DMA((SLOTS,)),
            pltpu.SemaphoreType.DMA((SLOTS,)),
            pltpu.SemaphoreType.DMA((SLOTS,)),
            pltpu.SemaphoreType.DMA((4,)),
        ],
        compiler_params=pltpu.CompilerParams(vmem_limit_bytes=63 * 1024 * 1024),
        cost_estimate=pl.CostEstimate(flops=6 * avg_rows * model_dim * ff_dim * 3 // 2, transcendentals=0,
                                      bytes_accessed=3 * num_loc * model_dim * ff_dim * 2),
        name='experts',
    )(counts, toks, gates, *segs, w_gate, w_up, w_down, *after)


def merge_kernel(blocks_half, num_pairs, *refs):
    base_ref, out_ref, sum_v = refs[0], refs[-2], refs[-1]
    rows = base_ref.shape[0]
    pieces = refs[1].shape[1]
    idx = pl.program_id(0)

    def add_up(side):
        total = refs[1 + side][...]
        for pair in range(1, num_pairs):
            total = total + refs[1 + 2 * pair + side][...]
        for row in range(rows):
            sum_v[row * SLAB:row * SLAB + pieces, :] = total[row]

    pl.when(idx < blocks_half)(lambda: add_up(0))
    pl.when(idx >= blocks_half)(lambda: add_up(1))
    for col in range(pieces):
        cols = slice(col * LANES, (col + 1) * LANES)
        out_ref[:, cols] = (base_ref[:, cols].astype(jnp.float32) + sum_v[pl.ds(col, rows, stride=SLAB), :]).astype(out_ref.dtype)


def merge(base, pairs, out_dtype):
    tok_dev, model_dim = base.shape
    pieces = pairs[0][0].shape[1]
    rows = 128
    blocks_half = tok_dev // rows // 2
    slab = (rows, pieces, LANES)
    flat_spec = pl.BlockSpec((rows, model_dim), lambda idx: (idx, 0))
    first_spec = pl.BlockSpec(slab, lambda idx: (jnp.minimum(idx, blocks_half - 1), 0, 0))
    second_spec = pl.BlockSpec(slab, lambda idx: (jnp.maximum(idx - blocks_half, 0), 0, 0))
    return pl.pallas_call(
        functools.partial(merge_kernel, blocks_half, len(pairs)),
        out_shape=jax.ShapeDtypeStruct((tok_dev, model_dim), out_dtype),
        grid=(tok_dev // rows,),
        in_specs=[flat_spec] + [first_spec, second_spec] * len(pairs),
        out_specs=flat_spec,
        scratch_shapes=[pltpu.VMEM((rows * SLAB, LANES), jnp.float32)],
        compiler_params=pltpu.CompilerParams(vmem_limit_bytes=62 * 1024 * 1024),
        cost_estimate=pl.CostEstimate(flops=tok_dev * model_dim * 8, transcendentals=0, bytes_accessed=tok_dev * model_dim * 16),
        name='add_up',
    )(base, *[part for pair in pairs for part in pair])


def routing_exchange(tok_rows, w_router, ids_loc):
    top_k = ids_loc.shape[1]
    num_exp = w_router.shape[1]
    logits = lax.dot_general(w_router, tok_rows, (((0,), (1,)), ((), ())), preferred_element_type=jnp.float32)
    ids = ids_loc.T
    exp_range = jnp.arange(num_exp, dtype=jnp.int32)[:, None]
    picked = jnp.stack([jnp.sum(jnp.where(ids[k][None, :] == exp_range, logits, 0.0), axis=0) for k in range(top_k)])
    gates = jax.nn.softmax(picked, axis=0)
    packed = jnp.concatenate([ids.astype(jnp.float32), gates], axis=0)
    return lax.all_gather(packed, 'ep')


def routing_tables(everyone, num_exp, group, list_cap):
    top_k, tok_dev = everyone.shape[1] // 2, everyone.shape[2]
    num_loc = num_exp // group
    half = tok_dev // 2
    me = lax.axis_index('ep')
    chip, core = me // 2, me % 2
    chips = group // 2
    order = [((chip + off) % chips) * 2 + side for off in range(chips) for side in (core, 1 - core)]
    rolled = [lax.dynamic_index_in_dim(everyone, src, 0, keepdims=False) for src in order]
    passes = [[(6, 0), (2, 1), (7, 0), (3, 1)],
              [(4, 0), (4, 1), (5, 0), (5, 1)],
              [(6, 1), (2, 0), (7, 1), (3, 0)],
              [(0, 0), (0, 1), (1, 0), (1, 1)]]
    num_segs = len(passes[0])
    halves = jnp.stack([rolled[src][:, side * half:(side + 1) * half] for segs in passes for src, side in segs])
    halves = halves.reshape(len(passes), 1, num_segs, 2 * top_k, half)
    mine = (me * num_loc + jnp.arange(num_loc, dtype=jnp.int32)).astype(jnp.float32)[None, :, None, None]
    columns = (len(passes), num_loc, num_segs, half)
    named = jnp.zeros(columns, jnp.bool_)
    gate = jnp.zeros(columns, jnp.float32)
    for k in range(top_k):
        hit = halves[:, :, :, k] == mine
        named = named | hit
        gate = gate + jnp.where(hit, halves[:, :, :, top_k + k], 0.0)
    counts = jnp.sum(named.astype(jnp.int32), axis=3).reshape(len(passes), num_loc * num_segs)
    place = jnp.arange(half, dtype=jnp.int32) + half * jnp.arange(num_segs, dtype=jnp.int32)[:, None]
    key = jnp.where(named, place[None, None], half * num_segs)
    flat = (len(passes) * num_loc * num_segs, half)
    key, gate = lax.sort((key.reshape(flat).T, gate.reshape(flat).T), dimension=0, num_keys=1, is_stable=False)
    lists = (len(passes), num_loc * num_segs * list_cap)
    return counts, key[:list_cap].T.reshape(lists), gate[:list_cap].T.reshape(lists)


def solution(mesh):
    group = mesh.shape['ep']
    row_spec = P(('dp', 'ep'), None)
    full_spec = P(None, None)
    expert_spec = P('ep', None, None)
    forward = [(dev, (dev + 2) % group) for dev in range(group)]
    backward = [(dev, (dev - 2) % group) for dev in range(group)]
    across = [(dev, dev ^ 1) for dev in range(group)]

    def send(array, route):
        return lax.ppermute(array, 'ep', route)

    def device_step(tok_rows, w_router, ids_loc, w_gate, w_up, w_down, shared_gate, shared_up, shared_down):
        tok_dev, model_dim = tok_rows.shape
        top_k = ids_loc.shape[1]
        num_exp = w_router.shape[1]
        half = tok_dev // 2
        pieces = model_dim // LANES
        list_cap = -(-capacity_of(tok_dev, top_k, num_exp) // 8) * 8
        slabs = tok_rows.reshape(tok_dev, pieces, LANES)
        own_a, own_b = slabs[:half], slabs[half:]
        everyone = routing_exchange(tok_rows, w_router, ids_loc)
        left_a = send(own_a, forward)
        right_b = send(own_b, backward)
        pair_a, pair_b = send(own_a, across), send(own_b, across)
        counts, toks, gates = routing_tables(everyone, num_exp, group, list_cap)

        def run(idx, segs, after):
            mine_a, mine_b, other_a, other_b = expert_pass(counts[idx], toks[idx], gates[idx], segs, w_gate, w_up, w_down, list_cap, after)
            return mine_a, mine_b, send(other_a, across), send(other_b, across)

        gate_act = jnp.dot(tok_rows, shared_gate, preferred_element_type=jnp.float32)
        up_act = jnp.dot(tok_rows, shared_up, preferred_element_type=jnp.float32)
        hidden = (jax.nn.silu(gate_act) * up_act).astype(jnp.bfloat16)
        shared_out = jnp.dot(hidden, shared_down, preferred_element_type=jnp.float32).astype(jnp.bfloat16)

        far_a, far_b = send(left_a, forward), send(right_b, backward)
        left_b, right_a = send(own_b, forward), send(own_a, backward)

        segs = [left_a, right_b, send(left_a, across), send(right_b, across)]
        mine_a, mine_b, other_a, other_b = run(0, segs, [hidden])
        to_left, to_right = mine_a + other_a, mine_b + other_b
        near_a, near_b = send(to_left, backward), send(to_right, forward)

        segs = [far_a, far_b, send(far_a, across), send(far_b, across)]
        mine_a, mine_b, other_a, other_b = run(1, segs, [to_left, to_right])
        to_right, to_left = mine_a + other_a, mine_b + other_b
        via_a, via_b = send(to_right, forward), send(to_left, backward)

        segs = [left_b, right_a, send(left_b, across), send(right_a, across)]
        mine_a, mine_b, other_a, other_b = run(2, segs, [to_left, to_right])
        to_left, to_right = mine_a + other_a + via_b, mine_b + other_b + via_a
        last_b, last_a = send(to_left, backward), send(to_right, forward)

        mine_a, mine_b, other_a, other_b = run(3, [own_a, own_b, pair_a, pair_b], [to_left, to_right, shared_out])
        total = merge(shared_out, [(near_a, near_b)], jnp.float32)
        return merge(total, [(mine_a, mine_b), (other_a, other_b), (last_a, last_b)], jnp.bfloat16)

    return jax.shard_map(device_step, mesh=mesh, in_specs=(row_spec, full_spec, row_spec, expert_spec, expert_spec, expert_spec, full_spec, full_spec, full_spec), out_specs=row_spec, check_vma=False)
```
